256 devices in a mesh: dp: 32 (over y, x, core), mp: 8 (over z).
Axes of the slice: x: 4, y: 4, z: 8, core: 2. Of those that a mesh axis runs over, the one named last changes fastest.
Arguments:
- ref_hidden: bfloat16 [2048, 2048], P('dp', 'mp'), may hold values from -80 to 80
- proxy_hidden: bfloat16 [2048, 2048], P('dp', 'mp'), may hold values from -80 to 80
- ref_gain: float32 [2048], replicated, may hold values from 0.5 to 1.5
- proxy_gain: float32 [2048], replicated, may hold values from 0.5 to 1.5
- ref_head: bfloat16 [2048, 128256], P(None, ('dp', 'mp')), may hold values from -16 to 16
- proxy_head: bfloat16 [2048, 128256], P(None, ('dp', 'mp')), may hold values from -16 to 16
- token_ids: int32 [2048], P('dp'), may hold values from 0 to 128255
- bucket_ids: int32 [2048], P(('dp', 'mp')), may hold values from 0 to 4095
- domain_of_bucket: int32 [4096], replicated, may hold values from 0 to 21
- prior_weights: float32 [22], replicated, may hold values from 0.01 to 0.1
Outputs:
- ref_loss: float32 [2048], P(('dp', 'mp'))
- proxy_loss: float32 [2048], P(('dp', 'mp'))
- bucket_excess: float32 [4096], P(('dp', 'mp'))
- domain_log_weights: float32 [22], replicated
The draws below stay inside these ranges and needn't reach their ends.
All inputs are finite; a program needn't handle non-finite values.
Results may differ from the reference program's by a relative error of at most 0.0035.
Values may be sent and summed in bfloat16 or wider, within the bound.
A program may use at most 64 MiB of HBM per device.

```python
import math
import jax
import jax.numpy as jnp
import numpy as np
from jax import lax

D = 2048
VOCAB = 128256
BUCKETS = 4096
DOMAINS = 22
TOKENS = 2048


def head_draw(key, which):
    weights = jax.random.normal(jax.random.fold_in(key, 11 + which), (D, VOCAB), jnp.float32) * (3.0 / math.sqrt(D))
    return weights.astype(jnp.bfloat16)


def hidden_draw(key, which):
    noise = jax.random.normal(jax.random.fold_in(key, 21 + which), (TOKENS, D), jnp.float32)
    scales = jnp.exp(jax.random.uniform(jax.random.fold_in(key, 31 + which), (TOKENS, 1), jnp.float32, 0.0, math.log(10.0)))
    values = noise
    return (values * scales).astype(jnp.bfloat16)


def draw_ref_hidden(key, part):
    return hidden_draw(key, 0)


def draw_proxy_hidden(key, part):
    return hidden_draw(key, 1)


def draw_ref_head(key, part):
    return head_draw(key, 0)


def draw_proxy_head(key, part):
    return head_draw(key, 1)


def set_ends(result, own_key, smallest, top_value):
    shape = result.shape
    place = [jax.random.randint(jax.random.fold_in(own_key, axis), (), 0, shape[axis]) for axis in range(len(shape))]
    result = result.at[tuple(place)].set(smallest)
    longest = shape.index(max(shape))
    place[longest] = (place[longest] + 1) % shape[longest]
    return result.at[tuple(place)].set(top_value)


def skewed_wide(own_key, shape, count, lean):
    loads = [min(1 << octave, count + 1 - (1 << octave)) * (1 << 20) // math.isqrt((1 << octave) ** lean) + 1 for octave in range((count + 1).bit_length()) if 1 << octave <= count]
    scale = 1 + sum(loads) // (1 << 30)
    grid = np.cumsum(np.array([max(1, weight // scale) for weight in loads]))
    pick = jax.random.randint(jax.random.fold_in(own_key, 1), shape, 0, int(grid[len(loads) - 1]))
    start = jnp.left_shift(1, jnp.searchsorted(jnp.asarray(grid, jnp.int32), pick, side="right").astype(jnp.int32))
    grade = start - 1 + jax.random.randint(jax.random.fold_in(own_key, 4), shape, 0, 1 << 30) % jnp.minimum(start, count + 1 - start)
    return jax.random.permutation(jax.random.fold_in(own_key, 2), count)[grade].astype(jnp.int32)


def setup_inputs(seed: int = 0) -> dict:
    key_list = jax.random.split(jax.random.key(seed), 11)
    ref_hidden = draw_ref_hidden(jax.random.fold_in(key_list[10], 71), 0)
    proxy_hidden = draw_proxy_hidden(jax.random.fold_in(key_list[10], 71), 0)
    ref_gain = jnp.clip(1.0 + 0.1 * jax.random.normal(key_list[2], (D,), jnp.float32), 0.5, 1.5)
    proxy_gain = jnp.clip(1.0 + 0.1 * jax.random.normal(key_list[3], (D,), jnp.float32), 0.5, 1.5)
    ref_head = draw_ref_head(jax.random.fold_in(key_list[10], 71), 0)
    proxy_head = draw_proxy_head(jax.random.fold_in(key_list[10], 71), 0)
    token_ids = set_ends(skewed_wide(key_list[6], (TOKENS,), VOCAB, 2), jax.random.fold_in(key_list[6], 3), 0, VOCAB - 1).astype(jnp.int32)
    bucket_ids = set_ends(jax.random.randint(key_list[7], (TOKENS,), 0, BUCKETS), jax.random.fold_in(key_list[7], 1), 0, BUCKETS - 1).astype(jnp.int32)
    domain_of_bucket = set_ends(jax.random.randint(key_list[8], (BUCKETS,), 0, DOMAINS), jax.random.fold_in(key_list[8], 1), 0, DOMAINS - 1).astype(jnp.int32)
    prior_weights = jnp.clip(jnp.exp(jax.random.uniform(key_list[9], (DOMAINS,), jnp.float32, math.log(0.01), math.log(0.1))), 0.01, 0.1)
    return {"ref_hidden": ref_hidden, "proxy_hidden": proxy_hidden, "ref_gain": ref_gain, "proxy_gain": proxy_gain, "ref_head": ref_head, "proxy_head": proxy_head, "token_ids": token_ids, "bucket_ids": bucket_ids, "domain_of_bucket": domain_of_bucket, "prior_weights": prior_weights}


def normalize(hidden, gain):
    values = hidden.astype(jnp.float32)
    scale = lax.rsqrt(lax.optimization_barrier(jnp.mean(values * values, -1, keepdims=True)) + 1e-05)
    return (values * scale * gain).astype(jnp.bfloat16)

def score(hidden, gain, head, token_ids):
    normed = normalize(hidden, gain)
    width = VOCAB // 32
    rows = normed.shape[0]

    def block_step(index, carry):
        top, total = carry
        piece = lax.dynamic_slice_in_dim(head, index * width, width, 1)
        logits = jnp.dot(normed, piece, preferred_element_type=jnp.float32)
        newtop = jnp.maximum(top, lax.optimization_barrier(jnp.max(logits, -1)))
        total = total * jnp.exp(top - newtop) + lax.optimization_barrier(jnp.sum(jnp.exp(logits - newtop[:, None]), -1))
        return (newtop, total)
    start = (jnp.full((rows,), -jnp.inf, jnp.float32), jnp.zeros((rows,), jnp.float32))
    top, total = lax.fori_loop(0, 32, block_step, start)
    columns = jnp.take(head, token_ids, axis=1)
    target = lax.optimization_barrier(jnp.sum(normed.astype(jnp.float32) * columns.T.astype(jnp.float32), -1))
    return top + jnp.log(total) - target

def reference(ref_hidden, proxy_hidden, ref_gain, proxy_gain, ref_head, proxy_head, token_ids, bucket_ids, domain_of_bucket, prior_weights):
    ref_loss = score(ref_hidden, ref_gain, ref_head, token_ids)
    proxy_loss = score(proxy_hidden, proxy_gain, proxy_head, token_ids)
    excess = jnp.maximum(proxy_loss - ref_loss, 0.0)
    bucket_sum = jax.ops.segment_sum(excess, bucket_ids, BUCKETS)
    bucket_count = jax.ops.segment_sum(jnp.ones_like(excess), bucket_ids, BUCKETS)
    bucket_excess = bucket_sum / jnp.maximum(bucket_count, 1.0)
    domain_sum = jax.ops.segment_sum(bucket_sum, domain_of_bucket, DOMAINS)
    domain_count = jax.ops.segment_sum(bucket_count, domain_of_bucket, DOMAINS)
    domain_excess = domain_sum / jnp.maximum(domain_count, 1.0)
    weights = jax.nn.softmax(jnp.log(prior_weights) + 1.0 * domain_excess)
    domain_log_weights = jnp.log(0.999 * weights + 0.001 / DOMAINS)
    return (ref_loss, proxy_loss, bucket_excess, domain_log_weights)
```

```python
import jax
import jax.numpy as jnp
from jax import lax
from jax.experimental import pallas as pl
from jax.experimental.pallas import tpu as pltpu
from jax.sharding import Mesh
from jax.sharding import PartitionSpec as P

DP_MP = ("dp_0", "dp_1", "dp_2", "mp")
DP = ("dp_0", "dp_1", "dp_2")
MESH = pl.DeviceIdType.MESH
NX, NY, NZ = 4, 4, 8
ROWS, FEAT = 64, 256
D = NZ * FEAT
BUCKETS, DOMAINS = 4096, 22
STEPS = ((1, 0, 0), (-1, 0, 0), (0, 1, 0), (0, -1, 0), (0, 0, 1), (0, 0, -1))
SENDS = (
    0, 256, 512, 768, 1024, 1280, 1664, 1920, 2176, 2432, 2688, 2944,
    7712, 7943, 8288, 8544, 8705, 8967, 9376, 9473, 9888, 10208, 10248, 10504,
    10753, 11143, 11296, 11649, 11800, 12056, 12295, 12673, 12935, 13191, 13441, 13703,
    13848, 14216, 14344, 14744, 14984, 15264, 15362, 15719, 15975, 16231, 16448, 16646,
    17064, 17154, 17505, 17761, 17922, 18279, 18472, 18841, 18946, 19206, 19648, 19960,
    19977, 20455, 20486, 20738, 21160, 21416, 21519, 21880, 22146, 22303, 22681, 22943,
    23046, 23301, 23557, 23813, 24129, 24391, 24579, 24835, 25190, 25442, 25705, 25861,
    26122, 26398, 26627, 26883, 27336, 27592, 27662, 28009, 28231, 28487, 28921, 29183,
    29322, 29561, 29830, 29977, 30401, 30663, 30733, 31077, 31333, 31589, 31810, 32101,
    32261, 32618, 32772, 33123, 33386, 33711, 33803, 34158, 34315, 34564, 35017, 35279,
    35332, 35710, 35853, 36162, 36602, 36862, 36887, 37254, 37390, 37658, 38082, 38342,
    38417, 38765, 38979, 39268, 39491, 39789, 39948, 40317, 40460, 40771, 41130, 41390,
    41491, 41858, 42062, 42328, 42698, 42958, 43024, 43406, 43593, 43871, 44186, 44541,
    44565, 44943, 45281, 45402, 45763, 45982, 46102, 46460, 46669, 46968, 47179, 47494,
    47636, 48010, 48203, 48506, 48770, 49069, 49170, 49425, 49773, 50046, 50314, 50637,
    50832, 50964, 51307, 51583, 51867, 52110, 52255, 52624, 52942, 53028, 53474, 53734,
    53787, 54268, 54348, 54565, 54840, 55173, 55322, 55801, 56008, 56102, 56554, 56814,
    56989, 57339, 57546, 57855, 57995, 58256, 58522, 58879, 59081, 59388, 59568, 59824,
    60063, 60413, 60619, 60926, 61168, 61413, 61598, 61944, 62156, 62461, 62608, 62934,
    63129, 63486, 63695, 63995, 64160, 64493, 64664, 65194, 65469, 65753, 65943, 66204,
    66731, 67066, 67258, 67511, 67717, 68268, 68508, 69031, 69252, 69773, 70043, 70289,
    70787, 71841,
)
PIECES = (
    (0, (0, 12, 1, 3), (21, 25, 26, 27)),
    (0, (4, 8, 13, 15), (28, 30, 30, 30)),
    (0, (2, 5, 9, 11), (31, 31, 35, 35)),
    (1, (15, 8, 5, 9), (33, 34, 36, 37)),
    (0, (6, 14, 10, 7), (37, 38, 40, 41)),
    (1, (3, 0, 1, 12), (38, 40, 42, 44)),
    (1, (10, 13, 11, 7), (46, 46, 47, 48)),
    (1, (14, 6, 2, 4), (48, 49, 50, 51)),
)
DOT_STEPS = 1


def moved(v, d):
    x, y, z = v // 32, v // 8 % 4, v % 8
    dx, dy, dz = STEPS[d]
    return ((x + dx) % NX * 4 + (y + dy) % NY) * 8 + (z + dz) % NZ


def plan():
    sends = [(c // 1536, c // 256 % 6, c // 128 % 2, c % 128) for c in SENDS]
    segments, at, arrived = [], 0, set()

    def need(m, v):
        if (m, v) in arrived:
            return []
        arrived.add((m, v))
        return [(m, v)]

    for m, cols, done in PIECES:
        ends = [*done, done[-1] + DOT_STEPS, done[-1] + 2 * DOT_STEPS]
        own = []
        for p, end in enumerate(ends):
            part = []
            while at < len(sends) and sends[at][0] < end:
                part += need(*sends[at][2:]) + [sends[at]]
                at += 1
            if p < 4:
                for vz in range(NZ):
                    part += need(m, cols[p] * NZ + vz)
            own.append(part)
        segments.append(own)
    assert at == len(sends)
    return segments


SEGMENTS = plan()
COUNTS = [sum(c // 256 % 6 == d for c in SENDS) for d in range(6)]


def pick(i, values):
    out = jnp.int32(values[0])
    for k in range(1, len(values)):
        out = jnp.where(i == k, jnp.int32(values[k]), out)
    return out


def kernel(
    hid0, hid1, gain0, gain1, head0, head1, tokens_in, buckets_in, table_in, prior_in,
    loss0, loss1, bucket_out, domain_out,
    buf, nb, hb, lg, gains, tokens, buckets, table, prior, tid, bid, brow, rows, bfull, st, r1, c1, r2, o3, r3,
    lsem, ssem, rsem, hsem, tsem, bsem, wsem, psem, s1, s2, s3,
):
    y, x, c, z = (lax.axis_index(a) for a in DP_MP)
    hidden, heads = (hid0, hid1), (head0, head1)
    vocab = head0.shape[0]

    def wrap(a, k, n):
        return lax.rem(a + (k + n) % n, n)

    xs = [wrap(x, -k, NX) for k in range(NX)]
    ys = [wrap(y, -k, NY) for k in range(NY)]
    zs = [wrap(z, -k, NZ) for k in range(NZ)]

    def slot(m, v):
        return (m * 16 + ys[v // 8 % 4] * 4 + xs[v // 32]) * 8 + zs[v % 8]

    def col_of(w):
        return ys[w % 4] * 4 + xs[w // 4]

    def at(a, b, cc, k):
        return (wrap(y, b, NY), wrap(x, a, NX), cc, wrap(z, k, NZ))

    other = 1 - c
    partner = (y, x, other, z)
    plane = [(a, b) for a in range(NX) for b in range(NY) if (a, b) != (0, 0)]
    column = list(range(1, NZ))
    me_col = y * 4 + x

    def remote(src, dst, ss, rs, dev):
        return pltpu.make_async_remote_copy(
            src_ref=src, dst_ref=dst, send_sem=ss, recv_sem=rs, device_id=dev, device_id_type=MESH
        )

    own_loads = [
        pltpu.make_async_copy(hidden[m], buf.at[slot(m, 0)], lsem.at[m]) for m in range(2)
    ]
    head_loads = [pltpu.make_async_copy(heads[m], hb.at[m, 0], lsem.at[2 + m]) for m in range(2)]
    small_loads = [
        pltpu.make_async_copy(src, dst, lsem.at[4 + k])
        for k, (src, dst) in enumerate(
            (
                (tokens_in, tokens),
                (buckets_in, buckets),
                (gain0, gains.at[0]),
                (gain1, gains.at[1]),
                (table_in, table),
                (prior_in, prior),
            )
        )
    ]
    for load in own_loads + small_loads:
        load.start()

    peers = [at(0, 0, c, k) for k in column]
    peers += [at(0, 0, other, k) for k in range(NZ)]
    peers += [at(a, b, c, 0) for a, b in plane]
    barrier = pltpu.get_barrier_semaphore()
    for peer in peers:
        pl.semaphore_signal(barrier, inc=1, device_id=peer, device_id_type=MESH)
    pl.semaphore_wait(barrier, len(peers))

    def run(ops):
        for op in ops:
            here = buf.at[slot(*op[-2:])]
            if len(op) == 2:
                m, v = op
                if v == 0:
                    own_loads[m].wait()
                else:
                    pltpu.make_async_copy(here, here, rsem.at[m * 128 + v]).wait()
            else:
                _, d, m, v = op
                dx, dy, dz = STEPS[d]
                there = rsem.at[m * 128 + moved(v, d)]
                remote(here, here, ssem.at[d], there, at(dx, dy, c, dz)).start()

    first = SEGMENTS[0][0]
    early = next(k for k, op in enumerate(first) if len(op) == 4 and op[0] >= 2) - 1
    run(first[:early])

    head_sends = [
        remote(heads[m], hb.at[m, 1], hsem.at[0, m], hsem.at[1, m], partner) for m in range(2)
    ]
    for m in range(2):
        head_sends[m].start()
        head_loads[m].start()
    token_sends = [
        remote(tokens, tid.at[me_col], tsem.at[0, a * 4 + b], tsem.at[1, a * 4 + b], at(a, b, c, 0))
        for a, b in plane
    ]
    bucket_sends = [
        remote(buckets, bid.at[z], bsem.at[0, k], bsem.at[1, k], at(0, 0, c, k)) for k in column
    ]
    for load in small_loads:
        load.wait()
    for copy in token_sends + bucket_sends:
        copy.start()
    tid[me_col] = tokens[...]
    bid[z] = buckets[...]
    st[...] = jnp.zeros(st.shape, jnp.float32)

    run(first[early:])

    for copy in bucket_sends:
        copy.wait()
    lane = lax.broadcasted_iota(jnp.int32, (1, 128), 1)
    packed = jnp.zeros((1, 128), jnp.int32)
    for k in range(NZ):
        wide = jnp.concatenate([bid[k]] * 16, axis=1)
        packed = packed + jnp.where(lane // 8 == k + 8 * lax.rem(x, 2), wide, 0)
    brow[...] = packed
    rows[me_col] = packed
    row_sends = [
        remote(brow, rows.at[me_col], wsem.at[0, a * 4 + b], wsem.at[1, a * 4 + b], at(a, b, c, 0))
        for a, b in plane
    ]
    for copy in row_sends:
        copy.start()
    for copy in token_sends:
        copy.wait()
    for copy in head_sends:
        copy.wait()
    for copy in head_loads:
        copy.wait()

    offset = ((me_col * 2 + c) * NZ + z) * vocab
    offset2 = ((me_col * 2 + other) * NZ + z) * vocab
    number = lax.broadcasted_iota(jnp.int32, (vocab, 4 * ROWS), 0)
    tile_row = lax.broadcasted_iota(jnp.int32, (8, 128), 0)
    tile_lane = lax.broadcasted_iota(jnp.int32, (8, 128), 1)
    cols_by_piece = [[col_of(w) for w in p[1]] for p in PIECES]

    def product(head, rows_):
        return lax.dot_general(
            head, rows_, (((1,), (1,)), ((), ())), preferred_element_type=jnp.float32
        )

    def chosen(i, values):
        out = values[0]
        for k in range(1, len(values)):
            out = jnp.where(i == k, values[k], out)
        return out

    def segment(i, p):
        for k in range(len(PIECES)):
            todo = [] if (k, p) == (0, 0) else SEGMENTS[k][p]

            @pl.when(i == k)
            def _(todo=todo):
                run(todo)

    def piece(i, _):
        m = pick(i, [p[0] for p in PIECES])
        cols = [chosen(i, [cs[k] for cs in cols_by_piece]) for k in range(4)]
        for k in range(4):
            segment(i, k)
            base = (m * 16 + cols[k]) * NZ
            total = jnp.zeros((ROWS, FEAT), jnp.float32)
            for f in range(NZ):
                values = buf[base + f].astype(jnp.float32)
                total = total + values * values
            scale = lax.rsqrt(jnp.sum(total, -1, keepdims=True) * (1.0 / D) + 1e-05)
            for f in range(NZ):
                values = buf[base + f].astype(jnp.float32)
                span = slice(f * FEAT, (f + 1) * FEAT)
                nb[k * ROWS : (k + 1) * ROWS, span] = (values * scale * gains[m, :, span]).astype(
                    jnp.bfloat16
                )
        lg[0] = product(hb[m, 0], nb[...])
        segment(i, 4)
        lg[1] = product(hb[m, 1], nb[...])
        ids = jnp.concatenate([tid[col] for col in cols], axis=1)
        left, right = lg[0], lg[1]
        top = jnp.max(jnp.maximum(left, right), 0, keepdims=True)
        sums = jnp.sum(jnp.exp(left - top) + jnp.exp(right - top), 0, keepdims=True)
        target = jnp.sum(
            jnp.where(number == ids - offset, left, 0.0)
            + jnp.where(number == ids - offset2, right, 0.0),
            0,
            keepdims=True,
        )
        partial = top + jnp.log(sums)
        for k, col in enumerate(cols):
            part = slice(k // 2 * 128, k // 2 * 128 + 128)
            both = jnp.where(tile_row % 2 == 0, partial[:, part], target[:, part])
            half = lax.rem(col, 2)
            mine = jnp.where(half == k % 2, both, pltpu.roll(both, 64, 1))
            keep = (tile_row // 2 == m) & (tile_lane // 64 == half)
            st[col // 2] = jnp.where(keep, mine, st[col // 2])
        segment(i, 5)
        return 0

    lax.fori_loop(0, len(PIECES), piece, 0)

    def merged(tiles):
        top = tiles[0]
        for t in tiles[1:]:
            top = jnp.maximum(top, t)
        total, plain = jnp.exp(tiles[0] - top), tiles[0]
        for t in tiles[1:]:
            total, plain = total + jnp.exp(t - top), plain + t
        return jnp.where(tile_row % 2 == 0, top + jnp.log(total), plain)

    first_sends = [
        remote(st.at[wrap(z, k, NZ)], r1.at[k], s1.at[0, k], s1.at[1, k], at(0, 0, c, k))
        for k in column
    ]
    for copy in first_sends:
        copy.start()
    for copy in row_sends:
        copy.wait()
    for q in range(NZ):
        bfull[c, q] = rows[2 * q] + rows[2 * q + 1]
    swap = remote(bfull.at[c], bfull.at[c], psem.at[0], psem.at[1], partner)
    swap.start()
    for d in range(6):
        sent = buf.at[pl.ds(0, COUNTS[d])]
        pltpu.make_async_copy(sent, sent, ssem.at[d]).wait()
    for k, copy in zip(column, first_sends):
        copy.wait()
    c1[...] = merged([st[z]] + [r1[k] for k in column])

    second_sends = [
        remote(c1, r2.at[a * 4 + b], s2.at[0, a * 4 + b], s2.at[1, a * 4 + b], at(a, b, c, 0))
        for a, b in plane
    ]
    for copy in second_sends:
        copy.start()
    swap.wait()
    bucket_rows = [bfull[j // NZ, j % NZ] for j in range(16)]
    low = lax.broadcasted_iota(jnp.int32, (128, 128), 0)
    high = lax.broadcasted_iota(jnp.int32, (32, 128), 0)
    small = table[...].astype(jnp.float32).astype(jnp.bfloat16)
    domain_rows = []
    for ids in bucket_rows:
        onehot = jnp.where(low == ids % 128, 1.0, 0.0).astype(jnp.bfloat16)
        found = jnp.dot(small, onehot, preferred_element_type=jnp.float32)
        domain_rows.append(
            jnp.sum(jnp.where(high == ids // 128, found, 0.0), 0, keepdims=True).astype(jnp.int32)
        )
    device = (me_col * 2 + c) * NZ + z
    bucket_number = lax.broadcasted_iota(jnp.int32, (16, 128), 0) + device * 16
    domain_number = lax.broadcasted_iota(jnp.int32, (24, 128), 0)
    bucket_hot = [bucket_number == ids for ids in bucket_rows]
    domain_hot = [domain_number == ids for ids in domain_rows]

    def counted(hot):
        total = jnp.zeros(hot[0].shape, jnp.float32)
        for h in hot:
            total = total + jnp.where(h, 1.0, 0.0)
        return jnp.maximum(jnp.sum(total, -1, keepdims=True), 1.0)

    bucket_count, domain_count = counted(bucket_hot), counted(domain_hot)
    for copy in second_sends:
        copy.wait()
    whole = merged([c1[...]] + [r2[a * 4 + b] for a, b in plane])
    low_loss, high_loss = whole[0:1] - whole[1:2], whole[2:3] - whole[3:4]
    o3[...] = jnp.zeros(o3.shape, jnp.float32)
    o3[0:1] = low_loss
    o3[1:2] = high_loss
    o3[2:3] = jnp.maximum(high_loss - low_loss, 0.0)

    place = c * NZ + z
    third_sends = [
        remote(o3, r3.at[place], s3.at[0, k], s3.at[1, k], at(0, 0, c, k)) for k in column
    ] + [
        remote(o3, r3.at[place], s3.at[0, 8 + k], s3.at[1, 8 + k], at(0, 0, other, k))
        for k in range(NZ)
    ]
    for copy in third_sends:
        copy.start()
    r3[place] = o3[...]
    for copy in third_sends:
        copy.wait()

    def summed(hot):
        total = jnp.zeros(hot[0].shape, jnp.float32)
        for j, h in enumerate(hot):
            total = total + jnp.where(h, r3[j, 2:3, :], 0.0)
        return jnp.sum(total, -1, keepdims=True)

    def along(values):
        n = values.shape[0]
        diagonal = lax.broadcasted_iota(jnp.int32, (n, 128), 0) == lax.broadcasted_iota(
            jnp.int32, (n, 128), 1
        )
        return jnp.sum(jnp.where(diagonal, values, 0.0), 0, keepdims=True)

    bucket_out[...] = along(summed(bucket_hot) / bucket_count)[:, :16]
    excess = along(summed(domain_hot) / domain_count)[:, :DOMAINS]
    scores = jnp.log(prior[...]) + 1.0 * excess
    raised = jnp.exp(scores - jnp.max(scores, -1, keepdims=True))
    weights = raised / jnp.sum(raised, -1, keepdims=True)
    domain_out[...] = jnp.log(0.999 * weights + 0.001 / DOMAINS)
    mine = r3[c * NZ + me_col // 2]
    begin = lax.rem(me_col, 2) * 64 + z * 8
    mine = pltpu.roll(mine, lax.rem(128 - begin, 128), 1)
    loss0[...] = mine[0:1, :8]
    loss1[...] = mine[1:2, :8]


def on_device(hid0, hid1, gain0, gain1, head0, head1, tokens, buckets, table, prior):
    vocab = head0.shape[1]
    anywhere = pl.BlockSpec(memory_space=pltpu.HBM)
    inside = pl.BlockSpec(memory_space=pltpu.VMEM)
    dma = pltpu.SemaphoreType.DMA
    f32, bf16, i32 = jnp.float32, jnp.bfloat16, jnp.int32
    outs = pl.pallas_call(
        kernel,
        out_shape=[
            jax.ShapeDtypeStruct((1, 8), f32),
            jax.ShapeDtypeStruct((1, 8), f32),
            jax.ShapeDtypeStruct((1, 16), f32),
            jax.ShapeDtypeStruct((1, DOMAINS), f32),
        ],
        in_specs=[anywhere] * 10,
        out_specs=[inside] * 4,
        scratch_shapes=[
            pltpu.VMEM((2 * 16 * NZ, ROWS, FEAT), bf16),
            pltpu.VMEM((4 * ROWS, D), bf16),
            pltpu.VMEM((2, 2, vocab, D), bf16),
            pltpu.VMEM((2, vocab, 4 * ROWS), f32),
            pltpu.VMEM((2, 1, D), f32),
            pltpu.VMEM((1, ROWS), i32),
            pltpu.VMEM((1, 8), i32),
            pltpu.VMEM((32, 128), i32),
            pltpu.VMEM((1, DOMAINS), f32),
            pltpu.VMEM((16, 1, ROWS), i32),
            pltpu.VMEM((NZ, 1, 8), i32),
            pltpu.VMEM((1, 128), i32),
            pltpu.VMEM((16, 1, 128), i32),
            pltpu.VMEM((2, NZ, 1, 128), i32),
            pltpu.VMEM((NZ, 8, 128), f32),
            pltpu.VMEM((NZ, 8, 128), f32),
            pltpu.VMEM((8, 128), f32),
            pltpu.VMEM((16, 8, 128), f32),
            pltpu.VMEM((8, 128), f32),
            pltpu.VMEM((16, 8, 128), f32),
            dma((10,)),
            dma((6,)),
            dma((256,)),
            dma((2, 2)),
            dma((2, 16)),
            dma((2, 8)),
            dma((2, 16)),
            dma((2,)),
            dma((2, 8)),
            dma((2, 16)),
            dma((2, 16)),
        ],
        compiler_params=pltpu.CompilerParams(
            collective_id=0, has_side_effects=True, vmem_limit_bytes=67_043_328
        ),
    )(
        hid0, hid1, gain0.reshape(1, D), gain1.reshape(1, D), head0.T, head1.T,
        tokens.reshape(1, ROWS), buckets.reshape(1, 8), table.reshape(32, 128),
        prior.reshape(1, DOMAINS),
    )
    return tuple(o.reshape(-1) for o in outs)


def solution(mesh):
    torus = Mesh(mesh.devices.reshape(NY, NX, 2, mesh.shape["mp"]), DP_MP)
    return jax.shard_map(
        on_device,
        mesh=torus,
        in_specs=(
            P(DP, "mp"),
            P(DP, "mp"),
            P(),
            P(),
            P(None, DP_MP),
            P(None, DP_MP),
            P(DP),
            P(DP_MP),
            P(),
            P(),
        ),
        out_specs=(P(DP_MP), P(DP_MP), P(DP_MP), P()),
        check_vma=False,
    )
```

```python
import jax
import jax.numpy as jnp
from jax import lax
from jax.experimental import pallas as pl
from jax.experimental.pallas import tpu as pltpu
from jax.sharding import Mesh
from jax.sharding import PartitionSpec as P

DP_MP = ("dp_0", "dp_1", "dp_2", "mp")
DP = ("dp_0", "dp_1", "dp_2")
MESH = pl.DeviceIdType.MESH
NX, NY, NZ = 4, 4, 8
ROWS, FEAT = 64, 256
D = NZ * FEAT
BUCKETS, DOMAINS = 4096, 22
STEPS = ((1, 0, 0), (-1, 0, 0), (0, 1, 0), (0, -1, 0), (0, 0, 1), (0, 0, -1), (0, 0, 2), (0, 0, -2))
STEPS += tuple(
    tuple(p + q for p, q in zip(STEPS[a], STEPS[b]))
    for a in range(6)
    for b in range(a + 1, 6)
    if a // 2 != b // 2
)
WAYS = len(STEPS)
SENDS = (
    0, 256, 512, 768, 1024, 1280, 6656, 6912, 7168, 8448, 12544, 13312,
    15488, 15744, 16000, 16256, 16512, 16768, 22144, 22400, 30727, 30977, 31233, 31489,
    31776, 32096, 35872, 36360, 36615, 37128, 40966, 41222, 41474, 41730, 41986, 42246,
    46082, 46338, 46598, 46854, 47224, 47480, 51256, 51560, 51752, 52088, 52264, 52520,
    56456, 56800, 57056, 57218, 57400, 57656, 61473, 61799, 61961, 62337, 62568, 62824,
    66712, 66968, 67208, 67359, 67714, 67992, 71683, 71939, 72197, 72453, 72707, 73062,
    76805, 77183, 77315, 77695, 77850, 78207, 81934, 82202, 82466, 82722, 83056, 83248,
    87097, 87310, 87562, 87846, 88112, 88392, 92208, 92518, 92770, 92958, 93249, 93632,
    97464, 97695, 97984, 98179, 98376, 98719, 102404, 102685, 102947, 103172, 103523, 103693,
    107549, 107803, 108069, 108414, 108736, 108895, 112698, 112909, 113163, 113443, 113777, 113975,
    117778, 118027, 118351, 118557, 119032, 119119, 122915, 123249, 123458, 123847, 124136, 124230,
    128158, 128414, 128712, 128922, 129179, 129438, 133132, 133501, 133644, 134013, 134360, 134525,
    138285, 138619, 138852, 139131, 139457, 139581, 143414, 143730, 144065, 144187, 144552, 144694,
    148523, 148836, 149191, 149403, 149753, 149959, 153753, 154011, 154344, 154526, 154857, 155103,
    158876, 159132, 159465, 159644, 159888, 160254, 163860, 164220, 164520, 164732, 165081, 165352,
    169117, 169331, 169549, 169887, 170178, 170317, 174234, 174467, 174786, 175005, 175273, 175528,
    179355, 179585, 179910, 180191, 180355, 180678, 184479, 184827, 185033, 185310, 185578, 185822,
    189590, 189948, 190121, 190458, 190624, 190854, 194706, 194951, 195311, 195420, 195720, 196079,
    199828, 200070, 200387, 200666, 200899, 201136, 204947, 205186, 205443, 205757, 205994, 206255,
    210050, 210326, 210629, 210939, 211171, 211360, 215172, 215444, 215686, 216027, 216299, 216534,
    220293, 220549, 220807, 221148, 225411, 225924, 226301, 226441, 226798, 230534, 231108, 236165,
    236715, 236974,
)
PIECES = (
    (0, (0, 1, 3, 4), (20, 26, 26, 26)),
    (0, (12, 2, 5, 15), (26, 32, 32, 32)),
    (0, (7, 13, 8, 6), (33, 33, 35, 38)),
    (1, (3, 15, 2, 7), (31, 37, 40, 42)),
    (0, (11, 14, 9, 10), (38, 38, 39, 44)),
    (1, (0, 11, 8, 6), (43, 43, 45, 46)),
    (1, (10, 12, 13, 14), (49, 49, 50, 50)),
    (1, (4, 9, 1, 5), (51, 51, 52, 52)),
)
DOT_STEPS = 0.5
AHEAD = 1


def moved(v, d):
    x, y, z = v // 32, v // 8 % 4, v % 8
    dx, dy, dz = STEPS[d]
    return ((x + dx) % NX * 4 + (y + dy) % NY) * 8 + (z + dz) % NZ


def plan():
    sends = [(c // (256 * WAYS), c // 256 % WAYS, c // 128 % 2, c % 128) for c in SENDS]
    segments, at, arrived = [], 0, set()

    def need(m, v):
        if (m, v) in arrived:
            return []
        arrived.add((m, v))
        return [(m, v)]

    for m, cols, done in PIECES:
        ends = [*done, *(done[-1] + DOT_STEPS * (q + 1) for q in range(5))]
        own = []
        for p, end in enumerate(ends):
            part = []
            while at < len(sends) and sends[at][0] < end + AHEAD:
                part += need(*sends[at][2:]) + [sends[at]]
                at += 1
            if p < 4:
                for vz in range(NZ):
                    part += need(m, cols[p] * NZ + vz)
            own.append(part)
        segments.append(own)
    assert at == len(sends)
    return segments


SEGMENTS = plan()
COUNTS = [sum(c // 256 % WAYS == d for c in SENDS) for d in range(WAYS)]


def pick(i, values):
    out = jnp.int32(values[0])
    for k in range(1, len(values)):
        out = jnp.where(i == k, jnp.int32(values[k]), out)
    return out


def kernel(
    hid0, hid1, gain0, gain1, head0, head1, tokens_in, buckets_in, table_in, prior_in,
    packed_out,
    buf, nb, hb, lg, gains, tokens, buckets, table, prior, tid, bid, brow, rows, bfull, st, r1, c1, r2, o3, r3,
    lsem, ssem, rsem, hsem, tsem, bsem, wsem, psem, s1, s2, s3,
):
    y, x, c, z = (lax.axis_index(a) for a in DP_MP)
    hidden, heads = (hid0, hid1), (head0, head1)
    vocab = head0.shape[0]

    def wrap(a, k, n):
        return lax.rem(a + (k + n) % n, n)

    xs = [wrap(x, -k, NX) for k in range(NX)]
    ys = [wrap(y, -k, NY) for k in range(NY)]
    zs = [wrap(z, -k, NZ) for k in range(NZ)]

    def slot(m, v):
        return (m * 16 + ys[v // 8 % 4] * 4 + xs[v // 32]) * 8 + zs[v % 8]

    def col_of(w):
        return ys[w % 4] * 4 + xs[w // 4]

    def at(a, b, cc, k):
        return (wrap(y, b, NY), wrap(x, a, NX), cc, wrap(z, k, NZ))

    other = 1 - c
    partner = (y, x, other, z)
    plane = [(a, b) for a in range(NX) for b in range(NY) if (a, b) != (0, 0)]
    column = list(range(1, NZ))
    me_col = y * 4 + x

    def remote(src, dst, ss, rs, dev):
        return pltpu.make_async_remote_copy(
            src_ref=src, dst_ref=dst, send_sem=ss, recv_sem=rs, device_id=dev, device_id_type=MESH
        )

    own_loads = [
        pltpu.make_async_copy(hidden[m], buf.at[slot(m, 0)], lsem.at[m]) for m in range(2)
    ]
    head_loads = [pltpu.make_async_copy(heads[m], hb.at[m, 0], lsem.at[2 + m]) for m in range(2)]
    small_loads = [
        pltpu.make_async_copy(src, dst, lsem.at[4 + k])
        for k, (src, dst) in enumerate(
            (
                (tokens_in, tokens),
                (buckets_in, buckets),
                (gain0, gains.at[0]),
                (gain1, gains.at[1]),
                (table_in, table),
                (prior_in, prior),
            )
        )
    ]
    for load in own_loads + small_loads:
        load.start()

    peers = [at(0, 0, c, k) for k in column]
    peers += [at(0, 0, other, k) for k in range(NZ)]
    peers += [at(a, b, c, 0) for a, b in plane]
    peers += [at(a, b, c, k) for a, b, k in STEPS if k and (a or b)]
    barrier = pltpu.get_barrier_semaphore()
    for peer in peers:
        pl.semaphore_signal(barrier, inc=1, device_id=peer, device_id_type=MESH)
    pl.semaphore_wait(barrier, len(peers))

    def run(ops):
        for op in ops:
            here = buf.at[slot(*op[-2:])]
            if len(op) == 2:
                m, v = op
                if v == 0:
                    own_loads[m].wait()
                else:
                    pltpu.make_async_copy(here, here, rsem.at[m * 128 + v]).wait()
            else:
                _, d, m, v = op
                dx, dy, dz = STEPS[d]
                there = rsem.at[m * 128 + moved(v, d)]
                remote(here, here, ssem.at[d], there, at(dx, dy, c, dz)).start()

    first = SEGMENTS[0][0]
    early = next(k for k, op in enumerate(first) if len(op) == 4 and op[0] >= 2) - 1
    run(first[:early])

    head_sends = [
        remote(heads[m], hb.at[m, 1], hsem.at[0, m], hsem.at[1, m], partner) for m in range(2)
    ]
    for m in range(2):
        head_sends[m].start()
        head_loads[m].start()
    token_sends = [
        remote(tokens, tid.at[me_col], tsem.at[0, a * 4 + b], tsem.at[1, a * 4 + b], at(a, b, c, 0))
        for a, b in plane
    ]
    bucket_sends = [
        remote(buckets, bid.at[z], bsem.at[0, k], bsem.at[1, k], at(0, 0, c, k)) for k in column
    ]
    for load in small_loads:
        load.wait()
    for copy in token_sends + bucket_sends:
        copy.start()
    tid[me_col] = tokens[...]
    bid[z] = buckets[...]
    st[...] = jnp.zeros(st.shape, jnp.float32)

    run(first[early:])

    for copy in bucket_sends:
        copy.wait()
    lane = lax.broadcasted_iota(jnp.int32, (1, 128), 1)
    packed = jnp.zeros((1, 128), jnp.int32)
    for k in range(NZ):
        wide = jnp.concatenate([bid[k]] * 16, axis=1)
        packed = packed + jnp.where(lane // 8 == k + 8 * lax.rem(x, 2), wide, 0)
    brow[...] = packed
    rows[me_col] = packed
    row_sends = [
        remote(brow, rows.at[me_col], wsem.at[0, a * 4 + b], wsem.at[1, a * 4 + b], at(a, b, c, 0))
        for a, b in plane
    ]
    for copy in row_sends:
        copy.start()
    for copy in token_sends:
        copy.wait()
    for copy in head_sends:
        copy.wait()
    for copy in head_loads:
        copy.wait()

    offset = ((me_col * 2 + c) * NZ + z) * vocab
    offset2 = ((me_col * 2 + other) * NZ + z) * vocab
    number = lax.broadcasted_iota(jnp.int32, (vocab, 4 * ROWS), 0)
    tile_row = lax.broadcasted_iota(jnp.int32, (8, 128), 0)
    tile_lane = lax.broadcasted_iota(jnp.int32, (8, 128), 1)
    cols_by_piece = [[col_of(w) for w in p[1]] for p in PIECES]

    def product(head, rows_):
        return lax.dot_general(
            head, rows_, (((1,), (1,)), ((), ())), preferred_element_type=jnp.float32
        )

    def chosen(i, values):
        out = values[0]
        for k in range(1, len(values)):
            out = jnp.where(i == k, values[k], out)
        return out

    def segment(i, p):
        for k in range(len(PIECES)):
            todo = [] if (k, p) == (0, 0) else SEGMENTS[k][p]

            @pl.when(i == k)
            def _(todo=todo):
                run(todo)

    def piece(i, _):
        m = pick(i, [p[0] for p in PIECES])
        cols = [chosen(i, [cs[k] for cs in cols_by_piece]) for k in range(4)]
        for k in range(4):
            segment(i, k)
            base = (m * 16 + cols[k]) * NZ
            total = jnp.zeros((ROWS, FEAT), jnp.float32)
            for f in range(NZ):
                values = buf[base + f].astype(jnp.float32)
                total = total + values * values
            scale = lax.rsqrt(jnp.sum(total, -1, keepdims=True) * (1.0 / D) + 1e-05)
            for f in range(NZ):
                values = buf[base + f].astype(jnp.float32)
                span = slice(f * FEAT, (f + 1) * FEAT)
                nb[k * ROWS : (k + 1) * ROWS, span] = (values * scale * gains[m, :, span]).astype(
                    jnp.bfloat16
                )
        for q in range(4):
            side, half = q // 2, slice(q % 2 * (D // 2), (q % 2 + 1) * (D // 2))
            part = product(hb[m, side, :, half], nb[:, half])
            lg[side] = part if q % 2 == 0 else lg[side] + part
            segment(i, 4 + q)
        ids = jnp.concatenate([tid[col] for col in cols], axis=1)
        left, right = lg[0], lg[1]
        top = jnp.max(jnp.maximum(left, right), 0, keepdims=True)
        sums = jnp.sum(jnp.exp(left - top) + jnp.exp(right - top), 0, keepdims=True)
        target = jnp.sum(
            jnp.where(number == ids - offset, left, 0.0)
            + jnp.where(number == ids - offset2, right, 0.0),
            0,
            keepdims=True,
        )
        partial = top + jnp.log(sums)
        for k, col in enumerate(cols):
            part = slice(k // 2 * 128, k // 2 * 128 + 128)
            both = jnp.where(tile_row % 2 == 0, partial[:, part], target[:, part])
            half = lax.rem(col, 2)
            mine = jnp.where(half == k % 2, both, pltpu.roll(both, 64, 1))
            keep = (tile_row // 2 == m) & (tile_lane // 64 == half)
            st[col // 2] = jnp.where(keep, mine, st[col // 2])
        segment(i, 8)
        return 0

    lax.fori_loop(0, len(PIECES), piece, 0)

    def merged(tiles):
        top = tiles[0]
        for t in tiles[1:]:
            top = jnp.maximum(top, t)
        total, plain = jnp.exp(tiles[0] - top), tiles[0]
        for t in tiles[1:]:
            total, plain = total + jnp.exp(t - top), plain + t
        return jnp.where(tile_row % 2 == 0, top + jnp.log(total), plain)

    first_sends = [
        remote(st.at[wrap(z, k, NZ)], r1.at[k], s1.at[0, k], s1.at[1, k], at(0, 0, c, k))
        for k in column
    ]
    for copy in first_sends:
        copy.start()
    for copy in row_sends:
        copy.wait()
    for q in range(NZ):
        bfull[c, q] = rows[2 * q] + rows[2 * q + 1]
    swap = remote(bfull.at[c], bfull.at[c], psem.at[0], psem.at[1], partner)
    swap.start()
    for d in range(WAYS):
        if COUNTS[d]:
            sent = buf.at[pl.ds(0, COUNTS[d])]
            pltpu.make_async_copy(sent, sent, ssem.at[d]).wait()
    for k, copy in zip(column, first_sends):
        copy.wait()
    c1[...] = merged([st[z]] + [r1[k] for k in column])

    second_sends = [
        remote(c1, r2.at[a * 4 + b], s2.at[0, a * 4 + b], s2.at[1, a * 4 + b], at(a, b, c, 0))
        for a, b in plane
    ]
    for copy in second_sends:
        copy.start()
    swap.wait()
    bucket_rows = [bfull[j // NZ, j % NZ] for j in range(16)]
    low = lax.broadcasted_iota(jnp.int32, (128, 128), 0)
    high = lax.broadcasted_iota(jnp.int32, (32, 128), 0)
    small = table[...].astype(jnp.float32).astype(jnp.bfloat16)
    domain_rows = []
    for ids in bucket_rows:
        onehot = jnp.where(low == ids % 128, 1.0, 0.0).astype(jnp.bfloat16)
        found = jnp.dot(small, onehot, preferred_element_type=jnp.float32)
        domain_rows.append(
            jnp.sum(jnp.where(high == ids // 128, found, 0.0), 0, keepdims=True).astype(jnp.int32)
        )
    device = (me_col * 2 + c) * NZ + z
    bucket_number = lax.broadcasted_iota(jnp.int32, (16, 128), 0) + device * 16
    domain_number = lax.broadcasted_iota(jnp.int32, (24, 128), 0)
    bucket_hot = [bucket_number == ids for ids in bucket_rows]
    domain_hot = [domain_number == ids for ids in domain_rows]

    def counted(hot):
        total = jnp.zeros(hot[0].shape, jnp.float32)
        for h in hot:
            total = total + jnp.where(h, 1.0, 0.0)
        return jnp.maximum(jnp.sum(total, -1, keepdims=True), 1.0)

    bucket_count, domain_count = counted(bucket_hot), counted(domain_hot)
    for copy in second_sends:
        copy.wait()
    whole = merged([c1[...]] + [r2[a * 4 + b] for a, b in plane])
    low_loss, high_loss = whole[0:1] - whole[1:2], whole[2:3] - whole[3:4]
    o3[...] = jnp.zeros(o3.shape, jnp.float32)
    o3[0:1] = low_loss
    o3[1:2] = high_loss
    o3[2:3] = jnp.maximum(high_loss - low_loss, 0.0)

    place = c * NZ + z
    third_sends = [
        remote(o3, r3.at[place], s3.at[0, k], s3.at[1, k], at(0, 0, c, k)) for k in column
    ] + [
        remote(o3, r3.at[place], s3.at[0, 8 + k], s3.at[1, 8 + k], at(0, 0, other, k))
        for k in range(NZ)
    ]
    for copy in third_sends:
        copy.start()
    r3[place] = o3[...]
    for copy in third_sends:
        copy.wait()

    def summed(hot):
        total = jnp.zeros(hot[0].shape, jnp.float32)
        for j, h in enumerate(hot):
            total = total + jnp.where(h, r3[j, 2:3, :], 0.0)
        return jnp.sum(total, -1, keepdims=True)

    def along(values):
        n = values.shape[0]
        diagonal = lax.broadcasted_iota(jnp.int32, (n, 128), 0) == lax.broadcasted_iota(
            jnp.int32, (n, 128), 1
        )
        return jnp.sum(jnp.where(diagonal, values, 0.0), 0, keepdims=True)

    packed_out[2:3] = along(summed(bucket_hot) / bucket_count)
    excess = along(summed(domain_hot) / domain_count)[:, :DOMAINS]
    scores = jnp.log(prior[...]) + 1.0 * excess
    raised = jnp.exp(scores - jnp.max(scores, -1, keepdims=True))
    weights = raised / jnp.sum(raised, -1, keepdims=True)
    packed_out[3:4, :DOMAINS] = jnp.log(0.999 * weights + 0.001 / DOMAINS)
    mine = r3[c * NZ + me_col // 2]
    begin = lax.rem(me_col, 2) * 64 + z * 8
    mine = pltpu.roll(mine, lax.rem(128 - begin, 128), 1)
    packed_out[0:2] = mine[0:2]


def unpack(packed, loss0, loss1, bucket_out, domain_out):
    loss0[...] = packed[0:1, :8]
    loss1[...] = packed[1:2, :8]
    bucket_out[...] = packed[2:3, :16]
    domain_out[...] = packed[3:4, :DOMAINS]


def on_device(hid0, hid1, gain0, gain1, head0, head1, tokens, buckets, table, prior):
    vocab = head0.shape[1]
    anywhere = pl.BlockSpec(memory_space=pltpu.HBM)
    inside = pl.BlockSpec(memory_space=pltpu.VMEM)
    dma = pltpu.SemaphoreType.DMA
    f32, bf16, i32 = jnp.float32, jnp.bfloat16, jnp.int32
    packed = pl.pallas_call(
        kernel,
        out_shape=jax.ShapeDtypeStruct((8, 128), f32),
        in_specs=[anywhere] * 10,
        out_specs=inside,
        scratch_shapes=[
            pltpu.VMEM((2 * 16 * NZ, ROWS, FEAT), bf16),
            pltpu.VMEM((4 * ROWS, D), bf16),
            pltpu.VMEM((2, 2, vocab, D), bf16),
            pltpu.VMEM((2, vocab, 4 * ROWS), f32),
            pltpu.VMEM((2, 1, D), f32),
            pltpu.VMEM((1, ROWS), i32),
            pltpu.VMEM((1, 8), i32),
            pltpu.VMEM((32, 128), i32),
            pltpu.VMEM((1, DOMAINS), f32),
            pltpu.VMEM((16, 1, ROWS), i32),
            pltpu.VMEM((NZ, 1, 8), i32),
            pltpu.VMEM((1, 128), i32),
            pltpu.VMEM((16, 1, 128), i32),
            pltpu.VMEM((2, NZ, 1, 128), i32),
            pltpu.VMEM((NZ, 8, 128), f32),
            pltpu.VMEM((NZ, 8, 128), f32),
            pltpu.VMEM((8, 128), f32),
            pltpu.VMEM((16, 8, 128), f32),
            pltpu.VMEM((8, 128), f32),
            pltpu.VMEM((16, 8, 128), f32),
            dma((10,)),
            dma((WAYS,)),
            dma((256,)),
            dma((2, 2)),
            dma((2, 16)),
            dma((2, 8)),
            dma((2, 16)),
            dma((2,)),
            dma((2, 8)),
            dma((2, 16)),
            dma((2, 16)),
        ],
        compiler_params=pltpu.CompilerParams(
            collective_id=0, has_side_effects=True, vmem_limit_bytes=67_043_328
        ),
    )(
        hid0, hid1, gain0.reshape(1, D), gain1.reshape(1, D), head0.T, head1.T,
        tokens.reshape(1, ROWS), buckets.reshape(1, 8), table.reshape(32, 128),
        prior.reshape(1, DOMAINS),
    )
    outs = pl.pallas_call(
        unpack,
        out_shape=[jax.ShapeDtypeStruct((1, n), f32) for n in (8, 8, 16, DOMAINS)],
    )(packed)
    return tuple(o.reshape(-1) for o in outs)


def solution(mesh):
    torus = Mesh(mesh.devices.reshape(NY, NX, 2, mesh.shape["mp"]), DP_MP)
    return jax.shard_map(
        on_device,
        mesh=torus,
        in_specs=(
            P(DP, "mp"),
            P(DP, "mp"),
            P(),
            P(),
            P(None, DP_MP),
            P(None, DP_MP),
            P(DP),
            P(DP_MP),
            P(),
            P(),
        ),
        out_specs=(P(DP_MP), P(DP_MP), P(DP_MP), P()),
        check_vma=False,
    )
```

```python
import jax
import jax.numpy as jnp
from jax import lax
from jax.experimental import pallas as pl
from jax.experimental.pallas import tpu as pltpu
from jax.sharding import Mesh
from jax.sharding import PartitionSpec as P

DP_MP = ("dp_0", "dp_1", "dp_2", "mp")
DP = ("dp_0", "dp_1", "dp_2")
MESH = pl.DeviceIdType.MESH
NX, NY, NZ = 4, 4, 8
ROWS, FEAT = 64, 256
D = NZ * FEAT
BUCKETS, DOMAINS = 4096, 22
STEPS = ((1, 0, 0), (-1, 0, 0), (0, 1, 0), (0, -1, 0), (0, 0, 1), (0, 0, -1), (0, 0, 2), (0, 0, -2))
STEPS += tuple(
    tuple(p + q for p, q in zip(STEPS[a], STEPS[b]))
    for a in range(6)
    for b in range(a + 1, 6)
    if a // 2 != b // 2
)
WAYS = len(STEPS)
SENDS = (
    0, 256, 512, 768, 1024, 1280, 6656, 6912, 7168, 8448, 12544, 13312,
    15488, 15744, 16000, 16256, 16512, 16768, 22144, 22400, 30727, 30977, 31233, 31489,
    31776, 32096, 35872, 36360, 36615, 37128, 40966, 41222, 41474, 41730, 41986, 42246,
    46082, 46338, 46598, 46854, 47224, 47480, 51256, 51560, 51752, 52088, 52264, 52520,
    56456, 56800, 57056, 57218, 57400, 57656, 61473, 61799, 61961, 62337, 62568, 62824,
    66712, 66968, 67208, 67359, 67714, 67992, 71683, 71939, 72197, 72453, 72707, 73062,
    76805, 77183, 77315, 77695, 77850, 78207, 81934, 82202, 82466, 82722, 83056, 83248,
    87097, 87310, 87562, 87846, 88112, 88392, 92208, 92518, 92770, 92958, 93249, 93632,
    97464, 97695, 97984, 98179, 98376, 98719, 102404, 102685, 102947, 103172, 103523, 103693,
    107549, 107803, 108069, 108414, 108736, 108895, 112698, 112909, 113163, 113443, 113777, 113975,
    117778, 118027, 118351, 118557, 119032, 119119, 122915, 123249, 123458, 123847, 124136, 124230,
    128158, 128414, 128712, 128922, 129179, 129438, 133132, 133501, 133644, 134013, 134360, 134525,
    138285, 138619, 138852, 139131, 139457, 139581, 143414, 143730, 144065, 144187, 144552, 144694,
    148523, 148836, 149191, 149403, 149753, 149959, 153753, 154011, 154344, 154526, 154857, 155103,
    158876, 159132, 159465, 159644, 159888, 160254, 163860, 164220, 164520, 164732, 165081, 165352,
    169117, 169331, 169549, 169887, 170178, 170317, 174234, 174467, 174786, 175005, 175273, 175528,
    179355, 179585, 179910, 180191, 180355, 180678, 184479, 184827, 185033, 185310, 185578, 185822,
    189590, 189948, 190121, 190458, 190624, 190854, 194706, 194951, 195311, 195420, 195720, 196079,
    199828, 200070, 200387, 200666, 200899, 201136, 204947, 205186, 205443, 205757, 205994, 206255,
    210050, 210326, 210629, 210939, 211171, 211360, 215172, 215444, 215686, 216027, 216299, 216534,
    220293, 220549, 220807, 221148, 225411, 225924, 226301, 226441, 226798, 230534, 231108, 236165,
    236715, 236974,
)
PIECES = (
    (0, (0, 1, 3, 4), (20, 26, 26, 26)),
    (0, (12, 2, 5, 15), (26, 32, 32, 32)),
    (0, (7, 13, 8, 6), (33, 33, 35, 38)),
    (1, (3, 15, 2, 7), (31, 37, 40, 42)),
    (0, (11, 14, 9, 10), (38, 38, 39, 44)),
    (1, (0, 11, 8, 6), (43, 43, 45, 46)),
    (1, (10, 12, 13, 14), (49, 49, 50, 50)),
    (1, (4, 9, 1, 5), (51, 51, 52, 52)),
)
DOT_STEPS = 0.5
AHEAD = 1


def moved(v, d):
    x, y, z = v // 32, v // 8 % 4, v % 8
    dx, dy, dz = STEPS[d]
    return ((x + dx) % NX * 4 + (y + dy) % NY) * 8 + (z + dz) % NZ


def plan():
    sends = [(c // (256 * WAYS), c // 256 % WAYS, c // 128 % 2, c % 128) for c in SENDS]
    segments, at, arrived = [], 0, set()

    def need(m, v):
        if (m, v) in arrived:
            return []
        arrived.add((m, v))
        return [(m, v)]

    for m, cols, done in PIECES:
        ends = [*done, *(done[-1] + DOT_STEPS * (q + 1) for q in range(5))]
        own = []
        for p, end in enumerate(ends):
            part = []
            while at < len(sends) and sends[at][0] < end + AHEAD:
                part += need(*sends[at][2:]) + [sends[at]]
                at += 1
            if p < 4:
                for vz in range(NZ):
                    part += need(m, cols[p] * NZ + vz)
            own.append(part)
        segments.append(own)
    assert at == len(sends)
    return segments


SEGMENTS = plan()
COUNTS = [sum(c // 256 % WAYS == d for c in SENDS) for d in range(WAYS)]


def pick(i, values):
    out = jnp.int32(values[0])
    for k in range(1, len(values)):
        out = jnp.where(i == k, jnp.int32(values[k]), out)
    return out


def kernel(
    hid0, hid1, gain0, gain1, head0, head1, tokens_in, buckets_in, table_in, prior_in,
    packed_out,
    buf, nb, hb, lg, gains, tokens, buckets, table, prior, tid, bid, brow, rows, bfull, st, r1, c1, r2, o3, r3,
    lsem, ssem, rsem, hsem, tsem, bsem, wsem, psem, s1, s2, s3,
):
    y, x, c, z = (lax.axis_index(a) for a in DP_MP)
    hidden, heads = (hid0, hid1), (head0, head1)
    vocab = head0.shape[0]

    def wrap(a, k, n):
        return lax.rem(a + (k + n) % n, n)

    xs = [wrap(x, -k, NX) for k in range(NX)]
    ys = [wrap(y, -k, NY) for k in range(NY)]
    zs = [wrap(z, -k, NZ) for k in range(NZ)]

    def slot(m, v):
        return (m * 16 + ys[v // 8 % 4] * 4 + xs[v // 32]) * 8 + zs[v % 8]

    def col_of(w):
        return ys[w % 4] * 4 + xs[w // 4]

    def at(a, b, cc, k):
        return (wrap(y, b, NY), wrap(x, a, NX), cc, wrap(z, k, NZ))

    other = 1 - c
    partner = (y, x, other, z)
    plane = [(a, b) for a in range(NX) for b in range(NY) if (a, b) != (0, 0)]
    plane.sort(key=lambda p: -min(p[0], NX - p[0]) - min(p[1], NY - p[1]))
    column = sorted(range(1, NZ), key=lambda k: -min(k, NZ - k))
    whole_column = sorted(range(NZ), key=lambda k: -min(k, NZ - k))
    me_col = y * 4 + x

    def remote(src, dst, ss, rs, dev):
        return pltpu.make_async_remote_copy(
            src_ref=src, dst_ref=dst, send_sem=ss, recv_sem=rs, device_id=dev, device_id_type=MESH
        )

    own_loads = [
        pltpu.make_async_copy(hidden[m], buf.at[slot(m, 0)], lsem.at[m]) for m in range(2)
    ]
    head_loads = [pltpu.make_async_copy(heads[m], hb.at[m, 0], lsem.at[2 + m]) for m in range(2)]
    small_loads = [
        pltpu.make_async_copy(src, dst, lsem.at[4 + k])
        for k, (src, dst) in enumerate(
            (
                (tokens_in, tokens),
                (buckets_in, buckets),
                (gain0, gains.at[0]),
                (gain1, gains.at[1]),
                (table_in, table),
                (prior_in, prior),
            )
        )
    ]
    for load in own_loads + small_loads:
        load.start()

    peers = [at(0, 0, c, k) for k in column]
    peers += [at(0, 0, other, k) for k in range(NZ)]
    peers += [at(a, b, c, 0) for a, b in plane]
    peers += [at(a, b, c, k) for a, b, k in STEPS if k and (a or b)]
    barrier = pltpu.get_barrier_semaphore()
    for peer in peers:
        pl.semaphore_signal(barrier, inc=1, device_id=peer, device_id_type=MESH)
    pl.semaphore_wait(barrier, len(peers))

    def run(ops):
        for op in ops:
            here = buf.at[slot(*op[-2:])]
            if len(op) == 2:
                m, v = op
                if v == 0:
                    own_loads[m].wait()
                else:
                    pltpu.make_async_copy(here, here, rsem.at[m * 128 + v]).wait()
            else:
                _, d, m, v = op
                dx, dy, dz = STEPS[d]
                there = rsem.at[m * 128 + moved(v, d)]
                remote(here, here, ssem.at[d], there, at(dx, dy, c, dz)).start()

    first = SEGMENTS[0][0]
    early = next(k for k, op in enumerate(first) if len(op) == 4 and op[0] >= 2) - 1
    run(first[:early])

    head_sends = [
        remote(heads[m], hb.at[m, 1], hsem.at[0, m], hsem.at[1, m], partner) for m in range(2)
    ]
    for m in range(2):
        head_sends[m].start()
        head_loads[m].start()
    token_sends = [
        remote(tokens, tid.at[me_col], tsem.at[0, a * 4 + b], tsem.at[1, a * 4 + b], at(a, b, c, 0))
        for a, b in plane
    ]
    bucket_sends = [
        remote(buckets, bid.at[z], bsem.at[0, k], bsem.at[1, k], at(0, 0, c, k)) for k in column
    ]
    for load in small_loads:
        load.wait()
    for copy in token_sends + bucket_sends:
        copy.start()
    tid[me_col] = tokens[...]
    bid[z] = buckets[...]
    st[...] = jnp.zeros(st.shape, jnp.float32)

    run(first[early:])

    for copy in bucket_sends:
        copy.wait()
    lane = lax.broadcasted_iota(jnp.int32, (1, 128), 1)
    packed = jnp.zeros((1, 128), jnp.int32)
    for k in range(NZ):
        wide = jnp.concatenate([bid[k]] * 16, axis=1)
        packed = packed + jnp.where(lane // 8 == k + 8 * lax.rem(x, 2), wide, 0)
    brow[...] = packed
    rows[me_col] = packed
    row_sends = [
        remote(brow, rows.at[me_col], wsem.at[0, a * 4 + b], wsem.at[1, a * 4 + b], at(a, b, c, 0))
        for a, b in plane
    ]
    for copy in row_sends:
        copy.start()
    for copy in token_sends:
        copy.wait()
    for copy in head_sends:
        copy.wait()
    for copy in head_loads:
        copy.wait()

    offset = ((me_col * 2 + c) * NZ + z) * vocab
    offset2 = ((me_col * 2 + other) * NZ + z) * vocab
    number = lax.broadcasted_iota(jnp.int32, (vocab, 4 * ROWS), 0)
    tile_row = lax.broadcasted_iota(jnp.int32, (8, 128), 0)
    tile_lane = lax.broadcasted_iota(jnp.int32, (8, 128), 1)
    cols_by_piece = [[col_of(w) for w in p[1]] for p in PIECES]

    def product(head, rows_):
        return lax.dot_general(
            head, rows_, (((1,), (1,)), ((), ())), preferred_element_type=jnp.float32
        )

    def chosen(i, values):
        out = values[0]
        for k in range(1, len(values)):
            out = jnp.where(i == k, values[k], out)
        return out

    def segment(i, p):
        for k in range(len(PIECES)):
            todo = [] if (k, p) == (0, 0) else SEGMENTS[k][p]

            @pl.when(i == k)
            def _(todo=todo):
                run(todo)

    def piece(i, _):
        m = pick(i, [p[0] for p in PIECES])
        cols = [chosen(i, [cs[k] for cs in cols_by_piece]) for k in range(4)]
        for k in range(4):
            segment(i, k)
            base = (m * 16 + cols[k]) * NZ
            total = jnp.zeros((ROWS, FEAT), jnp.float32)
            for f in range(NZ):
                values = buf[base + f].astype(jnp.float32)
                total = total + values * values
            scale = lax.rsqrt(jnp.sum(total, -1, keepdims=True) * (1.0 / D) + 1e-05)
            for f in range(NZ):
                values = buf[base + f].astype(jnp.float32)
                span = slice(f * FEAT, (f + 1) * FEAT)
                nb[k * ROWS : (k + 1) * ROWS, span] = (values * scale * gains[m, :, span]).astype(
                    jnp.bfloat16
                )
        for q in range(4):
            side, half = q // 2, slice(q % 2 * (D // 2), (q % 2 + 1) * (D // 2))
            part = product(hb[m, side, :, half], nb[:, half])
            lg[side] = part if q % 2 == 0 else lg[side] + part
            segment(i, 4 + q)
        ids = jnp.concatenate([tid[col] for col in cols], axis=1)
        left, right = lg[0], lg[1]
        top = jnp.max(jnp.maximum(left, right), 0, keepdims=True)
        sums = jnp.sum(jnp.exp(left - top) + jnp.exp(right - top), 0, keepdims=True)
        target = jnp.sum(
            jnp.where(number == ids - offset, left, 0.0)
            + jnp.where(number == ids - offset2, right, 0.0),
            0,
            keepdims=True,
        )
        partial = top + jnp.log(sums)
        for k, col in enumerate(cols):
            part = slice(k // 2 * 128, k // 2 * 128 + 128)
            both = jnp.where(tile_row % 2 == 0, partial[:, part], target[:, part])
            half = lax.rem(col, 2)
            mine = jnp.where(half == k % 2, both, pltpu.roll(both, 64, 1))
            keep = (tile_row // 2 == m) & (tile_lane // 64 == half)
            st[col // 2] = jnp.where(keep, mine, st[col // 2])
        segment(i, 8)
        return 0

    lax.fori_loop(0, len(PIECES), piece, 0)

    def merged(tiles):
        top = tiles[0]
        for t in tiles[1:]:
            top = jnp.maximum(top, t)
        total, plain = jnp.exp(tiles[0] - top), tiles[0]
        for t in tiles[1:]:
            total, plain = total + jnp.exp(t - top), plain + t
        return jnp.where(tile_row % 2 == 0, top + jnp.log(total), plain)

    first_sends = [
        remote(st.at[wrap(z, k, NZ)], r1.at[k], s1.at[0, k], s1.at[1, k], at(0, 0, c, k))
        for k in column
    ]
    for copy in first_sends:
        copy.start()
    for copy in row_sends:
        copy.wait()
    for q in range(NZ):
        bfull[c, q] = rows[2 * q] + rows[2 * q + 1]
    swap = remote(bfull.at[c], bfull.at[c], psem.at[0], psem.at[1], partner)
    swap.start()
    for d in range(WAYS):
        if COUNTS[d]:
            sent = buf.at[pl.ds(0, COUNTS[d])]
            pltpu.make_async_copy(sent, sent, ssem.at[d]).wait()
    swap.wait()
    bucket_rows = [bfull[j // NZ, j % NZ] for j in range(16)]
    low = lax.broadcasted_iota(jnp.int32, (128, 128), 0)
    high = lax.broadcasted_iota(jnp.int32, (32, 128), 0)
    small = table[...].astype(jnp.float32).astype(jnp.bfloat16)
    domain_rows = []
    for ids in bucket_rows:
        onehot = jnp.where(low == ids % 128, 1.0, 0.0).astype(jnp.bfloat16)
        found = jnp.dot(small, onehot, preferred_element_type=jnp.float32)
        domain_rows.append(
            jnp.sum(jnp.where(high == ids // 128, found, 0.0), 0, keepdims=True).astype(jnp.int32)
        )
    for copy in first_sends:
        copy.wait()
    c1[...] = merged([st[z]] + [r1[k] for k in column])

    second_sends = [
        remote(c1, r2.at[a * 4 + b], s2.at[0, a * 4 + b], s2.at[1, a * 4 + b], at(a, b, c, 0))
        for a, b in plane
    ]
    for copy in second_sends:
        copy.start()
    device = (me_col * 2 + c) * NZ + z
    bucket_number = lax.broadcasted_iota(jnp.int32, (16, 128), 0) + device * 16
    domain_number = lax.broadcasted_iota(jnp.int32, (24, 128), 0)
    bucket_hot = [bucket_number == ids for ids in bucket_rows]
    domain_hot = [domain_number == ids for ids in domain_rows]

    def counted(hot):
        total = jnp.zeros(hot[0].shape, jnp.float32)
        for h in hot:
            total = total + jnp.where(h, 1.0, 0.0)
        return jnp.maximum(jnp.sum(total, -1, keepdims=True), 1.0)

    bucket_count, domain_count = counted(bucket_hot), counted(domain_hot)
    for copy in second_sends:
        copy.wait()
    whole = merged([c1[...]] + [r2[a * 4 + b] for a, b in plane])
    low_loss, high_loss = whole[0:1] - whole[1:2], whole[2:3] - whole[3:4]
    o3[...] = jnp.zeros(o3.shape, jnp.float32)
    o3[0:1] = low_loss
    o3[1:2] = high_loss
    o3[2:3] = jnp.maximum(high_loss - low_loss, 0.0)

    place = c * NZ + z
    third_sends = [
        remote(o3, r3.at[place], s3.at[0, k], s3.at[1, k], at(0, 0, c, k)) for k in column
    ] + [
        remote(o3, r3.at[place], s3.at[0, 8 + k], s3.at[1, 8 + k], at(0, 0, other, k))
        for k in whole_column
    ]
    for copy in third_sends:
        copy.start()
    r3[place] = o3[...]
    for copy in third_sends:
        copy.wait()

    def summed(hot):
        total = jnp.zeros(hot[0].shape, jnp.float32)
        for j, h in enumerate(hot):
            total = total + jnp.where(h, r3[j, 2:3, :], 0.0)
        return jnp.sum(total, -1, keepdims=True)

    def along(values):
        n = values.shape[0]
        diagonal = lax.broadcasted_iota(jnp.int32, (n, 128), 0) == lax.broadcasted_iota(
            jnp.int32, (n, 128), 1
        )
        return jnp.sum(jnp.where(diagonal, values, 0.0), 0, keepdims=True)

    packed_out[2:3] = along(summed(bucket_hot) / bucket_count)
    excess = along(summed(domain_hot) / domain_count)[:, :DOMAINS]
    scores = jnp.log(prior[...]) + 1.0 * excess
    raised = jnp.exp(scores - jnp.max(scores, -1, keepdims=True))
    weights = raised / jnp.sum(raised, -1, keepdims=True)
    packed_out[3:4, :DOMAINS] = jnp.log(0.999 * weights + 0.001 / DOMAINS)
    mine = r3[c * NZ + me_col // 2]
    begin = lax.rem(me_col, 2) * 64 + z * 8
    mine = pltpu.roll(mine, lax.rem(128 - begin, 128), 1)
    packed_out[0:2] = mine[0:2]


def unpack(packed, loss0, loss1, bucket_out, domain_out):
    loss0[...] = packed[0:1, :8]
    loss1[...] = packed[1:2, :8]
    bucket_out[...] = packed[2:3, :16]
    domain_out[...] = packed[3:4, :DOMAINS]


def on_device(hid0, hid1, gain0, gain1, head0, head1, tokens, buckets, table, prior):
    vocab = head0.shape[1]
    anywhere = pl.BlockSpec(memory_space=pltpu.HBM)
    inside = pl.BlockSpec(memory_space=pltpu.VMEM)
    dma = pltpu.SemaphoreType.DMA
    f32, bf16, i32 = jnp.float32, jnp.bfloat16, jnp.int32
    packed = pl.pallas_call(
        kernel,
        out_shape=jax.ShapeDtypeStruct((8, 128), f32),
        in_specs=[anywhere] * 10,
        out_specs=inside,
        scratch_shapes=[
            pltpu.VMEM((2 * 16 * NZ, ROWS, FEAT), bf16),
            pltpu.VMEM((4 * ROWS, D), bf16),
            pltpu.VMEM((2, 2, vocab, D), bf16),
            pltpu.VMEM((2, vocab, 4 * ROWS), f32),
            pltpu.VMEM((2, 1, D), f32),
            pltpu.VMEM((1, ROWS), i32),
            pltpu.VMEM((1, 8), i32),
            pltpu.VMEM((32, 128), i32),
            pltpu.VMEM((1, DOMAINS), f32),
            pltpu.VMEM((16, 1, ROWS), i32),
            pltpu.VMEM((NZ, 1, 8), i32),
            pltpu.VMEM((1, 128), i32),
            pltpu.VMEM((16, 1, 128), i32),
            pltpu.VMEM((2, NZ, 1, 128), i32),
            pltpu.VMEM((NZ, 8, 128), f32),
            pltpu.VMEM((NZ, 8, 128), f32),
            pltpu.VMEM((8, 128), f32),
            pltpu.VMEM((16, 8, 128), f32),
            pltpu.VMEM((8, 128), f32),
            pltpu.VMEM((16, 8, 128), f32),
            dma((10,)),
            dma((WAYS,)),
            dma((256,)),
            dma((2, 2)),
            dma((2, 16)),
            dma((2, 8)),
            dma((2, 16)),
            dma((2,)),
            dma((2, 8)),
            dma((2, 16)),
            dma((2, 16)),
        ],
        compiler_params=pltpu.CompilerParams(
            collective_id=0, has_side_effects=True, vmem_limit_bytes=67_043_328
        ),
    )(
        hid0, hid1, gain0.reshape(1, D), gain1.reshape(1, D), head0.T, head1.T,
        tokens.reshape(1, ROWS), buckets.reshape(1, 8), table.reshape(32, 128),
        prior.reshape(1, DOMAINS),
    )
    outs = pl.pallas_call(
        unpack,
        out_shape=[jax.ShapeDtypeStruct((1, n), f32) for n in (8, 8, 16, DOMAINS)],
    )(packed)
    return tuple(o.reshape(-1) for o in outs)


def solution(mesh):
    torus = Mesh(mesh.devices.reshape(NY, NX, 2, mesh.shape["mp"]), DP_MP)
    return jax.shard_map(
        on_device,
        mesh=torus,
        in_specs=(
            P(DP, "mp"),
            P(DP, "mp"),
            P(),
            P(),
            P(None, DP_MP),
            P(None, DP_MP),
            P(DP),
            P(DP_MP),
            P(),
            P(),
        ),
        out_specs=(P(DP_MP), P(DP_MP), P(DP_MP), P()),
        check_vma=False,
    )
```
